32 devices in a mesh: section: 4 (over y, x), ctx: 8 (over z, core).
Axes of the slice: x: 2, y: 2, z: 4, core: 2. Of those that a mesh axis runs over, the one named last changes fastest.
Arguments:
- queries: bfloat16 [4, 8, 1024, 512], P('section', None, 'ctx'), may hold values from -5 to 5
- keys: bfloat16 [4, 8, 1024, 128], P('section', None, 'ctx'), may hold values from -5 to 5
- values: bfloat16 [4, 8, 1024, 128], P('section', None, 'ctx'), may hold values from -6 to 6
- out_grad: bfloat16 [4, 1024, 512], P('section', 'ctx'), may hold values from -6 to 6
- stretch_ids: int32 [16], P('ctx'), may hold values from 0 to 15, as said below
- stash_slot: int32 [4], P('section'), may hold values from 0 to 7
Outputs:
- passed_grads: bfloat16 [4, 1024, 768], P('section', 'ctx')
The draws below stay inside these ranges and needn't reach their ends.
Inputs may be any that keep to these rules, and one draw needn't show every extreme that they name: `stretch_ids`: for each sequence, the entries of its 8 row blocks (two a block, blocks in order) are a permutation of 0 to 15 in which a block's two entries are some c and 15 - c, in either order.
All inputs are finite; a program needn't handle non-finite values.
Results may differ from the reference program's by a relative error of at most 0.035.
Values may be sent and summed in bfloat16 or wider, within the bound.
A program may use at most 64 MiB of HBM per device.

```python
import math
import jax
import jax.numpy as jnp
from jax import lax

GROUP = 4
HEAD = 128
TOK_DEV = 128
SEQS = 1
MICRO = 8
HALF = 64
SPAN = 8
STRETCHES = 16
TOKENS = 1024
LENGTH = 1024
SECTIONS = 4
QW = 512


def draw_queries(key, part):
    shape = (SECTIONS, MICRO, TOKENS, GROUP * HEAD)
    return jax.random.truncated_normal(jax.random.fold_in(key, 7), -5.0, 5.0, shape, jnp.float32).astype(jnp.bfloat16)


def draw_keys(key, part):
    shape = (SECTIONS, MICRO, TOKENS, HEAD)
    return jax.random.truncated_normal(jax.random.fold_in(key, 17), -5.0, 5.0, shape, jnp.float32).astype(jnp.bfloat16)


def sequence_stretches(seq_key):
    order = jax.random.permutation(jax.random.fold_in(seq_key, 1), SPAN).astype(jnp.int32)
    flips = jax.random.randint(jax.random.fold_in(seq_key, 2), (SPAN,), 0, 2).astype(jnp.int32)
    mirror = (2 * SPAN - 1 - order).astype(jnp.int32)
    first = jnp.where(flips == 1, mirror, order)
    second = jnp.where(flips == 1, order, mirror)
    return jnp.stack([first, second], axis=1).astype(jnp.int32)


def draw_stretch_ids(key, part):
    seq_keys = jax.random.split(jax.random.fold_in(key, 11), SEQS)
    per_seq = jax.vmap(sequence_stretches)(seq_keys)
    return jnp.swapaxes(per_seq, 0, 1).reshape(STRETCHES).astype(jnp.int32)


def place_ends(entries, key, smallest, largest):
    spot = [jax.random.randint(jax.random.fold_in(key, axis), (), 0, length) for axis, length in enumerate(entries.shape)]
    main_axis = entries.shape.index(max(entries.shape))
    neighbour = spot[:main_axis] + [(spot[main_axis] + 1) % entries.shape[main_axis]] + spot[main_axis + 1:]
    return entries.at[tuple(spot)].set(smallest).at[tuple(neighbour)].set(largest)


def steps_of(own_key, shape, cuts, smallest, high):
    loudness, own = 1.0, jax.random.fold_in(own_key, 6)
    for axis_at, shards_of in cuts:
        draws = jnp.exp(jax.random.uniform(jax.random.fold_in(own, axis_at), (shards_of,), jnp.float32, smallest / len(cuts), high / len(cuts)))
        loudness = loudness * jnp.repeat(draws, shape[axis_at] // shards_of).reshape([-1 if axis == axis_at else 1 for axis in range(len(shape))])
    return loudness


def bell_draw(rng, extent, width, most, shards=(), kind=jnp.bfloat16):
    level = steps_of(rng, extent, shards, -0.22, 0.18) if shards else 1.0
    result = jax.random.normal(rng, extent, jnp.float32) * width * level
    return jnp.minimum(jnp.maximum(result, -most), most).astype(kind)


def setup_inputs(seed: int = 0) -> dict:
    splits = jax.random.split(jax.random.key(seed), 7)
    queries = draw_queries(jax.random.fold_in(splits[6], 71), 0)
    keys = draw_keys(jax.random.fold_in(splits[6], 71), 0)
    values = bell_draw(splits[2], (SECTIONS, MICRO, TOKENS, HEAD), 1.0, 6.0, ((0, 4), (2, 8)))
    out_grad = bell_draw(splits[3], (SECTIONS, TOKENS, QW), 1.0, 6.0, ((0, 4), (1, 8)))
    stretch_ids = draw_stretch_ids(jax.random.fold_in(splits[6], 71), 0)
    stash_slot = place_ends(jax.random.randint(splits[5], (SECTIONS,), 0, MICRO), jax.random.fold_in(splits[5], 1), 0, MICRO - 1).astype(jnp.int32)
    return dict(queries=queries, keys=keys, values=values, out_grad=out_grad, stretch_ids=stretch_ids, stash_slot=stash_slot)


def section_message(query_all, key_all, value_all, grad_all, token_place):
    softmax_scale = 1.0 / math.sqrt(HEAD)
    block_width = math.gcd(LENGTH, 256)
    blocks = LENGTH // block_width
    key_wide = key_all.astype(jnp.float32)
    value_wide = value_all.astype(jnp.float32)

    def one_block(sums_now, block_index):
        start = block_index * block_width
        query_rows = lax.dynamic_slice_in_dim(query_all, start, block_width, 0).astype(jnp.float32).reshape(block_width, GROUP, HEAD)
        grad_rows = lax.dynamic_slice_in_dim(grad_all, start, block_width, 0).astype(jnp.float32).reshape(block_width, GROUP, HEAD)
        query_place = lax.dynamic_slice_in_dim(token_place, start, block_width, 0)
        visible = token_place[None, None, :] <= query_place[:, None, None]
        scores = jnp.einsum('thd,cd->thc', query_rows, key_wide) * softmax_scale
        scores = jnp.where(visible, scores, -jnp.inf)
        row_top = lax.optimization_barrier(jnp.max(scores, axis=2, keepdims=True))
        log_total = row_top + jnp.log(lax.optimization_barrier(jnp.sum(jnp.exp(scores - row_top), axis=2, keepdims=True)))
        weights = jnp.exp(scores - log_total)
        probs_half = lax.optimization_barrier(weights.astype(jnp.bfloat16)).astype(jnp.float32)
        attention = jnp.einsum('thc,cd->thd', probs_half, value_wide)
        row_delta = lax.optimization_barrier(jnp.sum(grad_rows * attention, axis=2, keepdims=True))
        prob_grad = jnp.einsum('thd,cd->thc', grad_rows, value_wide)
        score_grad = lax.optimization_barrier((softmax_scale * weights * (prob_grad - row_delta)).astype(jnp.bfloat16)).astype(jnp.float32)
        query_grad = jnp.einsum('thc,cd->thd', score_grad, key_wide)
        key_grad = sums_now[0] + jnp.einsum('thc,thd->cd', score_grad, query_rows)
        value_grad = sums_now[1] + jnp.einsum('thc,thd->cd', probs_half, grad_rows)
        return ((key_grad, value_grad), query_grad.reshape(block_width, GROUP * HEAD))
    zero_rows = jnp.zeros((LENGTH, HEAD), jnp.float32)
    final_sums, query_grad = lax.scan(one_block, (zero_rows, zero_rows), jnp.arange(blocks, dtype=jnp.int32))
    query_grad = query_grad.reshape(LENGTH, GROUP * HEAD)
    return jnp.concatenate([query_grad, final_sums[0], final_sums[1]], axis=1).astype(jnp.bfloat16)

def regroup(array):
    tail = array.shape[1:]
    return jnp.swapaxes(array.reshape((SPAN, SEQS, TOK_DEV) + tail), 0, 1).reshape((SEQS, LENGTH) + tail)

def ungroup(array):
    tail = array.shape[2:]
    return jnp.swapaxes(array.reshape((SEQS, SPAN, TOK_DEV) + tail), 0, 1).reshape((TOKENS,) + tail)

def reference(queries, keys, values, out_grad, stretch_ids, stash_slot):
    row_ids = jnp.arange(TOKENS, dtype=jnp.int32)
    token_place = regroup(stretch_ids[row_ids // HALF] * HALF + row_ids % HALF)

    def per_section(section_index):
        stash_index = stash_slot[section_index]
        query_seq = regroup(queries[section_index, stash_index])
        key_seq = regroup(keys[section_index, stash_index])
        value_seq = regroup(values[section_index, stash_index])
        grad_seq = regroup(out_grad[section_index])

        def per_sequence(seq_index):
            return section_message(query_seq[seq_index], key_seq[seq_index], value_seq[seq_index], grad_seq[seq_index], token_place[seq_index])
        return ungroup(lax.map(per_sequence, jnp.arange(SEQS, dtype=jnp.int32)))
    messages = lax.map(per_section, jnp.arange(SECTIONS, dtype=jnp.int32))
    return jnp.roll(messages, -1, axis=0)
```

```python
import functools
import math

import jax
import jax.numpy as jnp
from jax import lax
from jax.experimental import pallas as pl
from jax.experimental.pallas import tpu as pltpu
from jax.sharding import PartitionSpec as P

MESH = pl.DeviceIdType.MESH
LOG2E = 1.4426950408889634
hidden = -1e30


def dot(a, b, dims):
    return lax.dot_general(a, b, (dims, ((), ())), preferred_element_type=jnp.float32)


def paired_chip(chip, offset, chips):
    if chips & (chips - 1):
        return lax.rem(2 * chips + offset - chip, chips)
    result = chip
    bit = 1
    while bit < chips:
        result = result + ((offset // bit) % 2) * bit * (1 - 2 * ((chip // bit) % 2))
        bit *= 2
    return result


def over(count, body, backwards=False):
    if count <= 4:
        for step in reversed(range(count)) if backwards else range(count):
            body(step)
    else:
        lax.fori_loop(
            0, count, lambda i, c: (body(count - 1 - i if backwards else i), c)[1], 0
        )


def kernel(
    n,
    sections,
    kv_ref,
    q_hbm,
    g_hbm,
    out_ref,
    q_in,
    g_in,
    q_rows,
    g_rows,
    q_turned,
    g_turned,
    kv_all,
    exps,
    dprobs,
    tops,
    row_top,
    row_total,
    row_delta,
    dq_turned,
    own_part,
    pair_send,
    pair_recv,
    sum_send,
    sum_recv,
    message,
    load_sem,
    kv_send_sem,
    kv_pass_sem,
    kv_recv_sem,
    pair_send_sem,
    pair_recv_sem,
    sum_send_sem,
    sum_recv_sem,
    relay_send_sem,
    relay_recv_sem,
):
    chips = n // 2
    rows = kv_ref.shape[0] - 16
    head = kv_ref.shape[1] // 2
    group = q_hbm.shape[1] // head
    half = rows // 2
    scale = 1.0 / math.sqrt(head)
    me = lax.axis_index("ctx")
    section = lax.axis_index("section")
    core = lax.rem(me, 2)
    chip = me // 2
    partner = 2 * chip + 1 - core
    before = lax.rem(section + sections - 1, sections)
    after = lax.rem(section + 1, sections)

    def peer(offset):
        return paired_chip(chip, offset, chips)

    load_q = pltpu.make_async_copy(q_hbm, q_in, load_sem.at[0])
    load_g = pltpu.make_async_copy(g_hbm, g_in, load_sem.at[1])
    load_q.start()
    load_g.start()

    barrier = pltpu.get_barrier_semaphore()
    pl.semaphore_signal(barrier, inc=1, device_id=(section, partner), device_id_type=MESH)
    for o in range(1, chips):
        pl.semaphore_signal(
            barrier, inc=1, device_id=(section, 2 * peer(o) + core), device_id_type=MESH
        )
    pl.semaphore_signal(barrier, inc=1, device_id=(before, me), device_id_type=MESH)
    pl.semaphore_signal(barrier, inc=1, device_id=(after, me), device_id_type=MESH)

    load_q.wait()
    load_g.wait()
    for h in range(group):
        at = slice(h * rows, (h + 1) * rows)
        col = slice(h * head, (h + 1) * head)
        q_rows[at, :] = q_in[:, col]
        g_rows[at, :] = g_in[:, col]
        q_turned[:, at] = q_in[:, col].T
        g_turned[:, at] = g_in[:, col].T
    kv_all[me] = kv_ref[...]

    pl.semaphore_wait(barrier, chips + 2)

    def kv_copy(o):
        return pltpu.make_async_remote_copy(
            src_ref=kv_ref,
            dst_ref=kv_all.at[me],
            send_sem=kv_send_sem.at[o],
            recv_sem=kv_recv_sem.at[me],
            device_id=(section, 2 * peer(o) + core),
            device_id_type=MESH,
        )

    def kv_partner():
        return pltpu.make_async_remote_copy(
            src_ref=kv_ref,
            dst_ref=kv_all.at[me],
            send_sem=kv_send_sem.at[0],
            recv_sem=kv_recv_sem.at[me],
            device_id=(section, partner),
            device_id_type=MESH,
        )

    def kv_pass(o):
        origin = 2 * peer(o) + core
        return pltpu.make_async_remote_copy(
            src_ref=kv_all.at[origin],
            dst_ref=kv_all.at[origin],
            send_sem=kv_pass_sem.at[o],
            recv_sem=kv_recv_sem.at[origin],
            device_id=(section, partner),
            device_id_type=MESH,
        )

    def kv_arrived(origin):
        pltpu.make_async_remote_copy(
            src_ref=kv_ref,
            dst_ref=kv_all.at[origin],
            send_sem=kv_send_sem.at[0],
            recv_sem=kv_recv_sem.at[origin],
            device_id=(section, partner),
            device_id_type=MESH,
        ).wait_recv()

    kv_partner().start()
    for o in range(1, chips):
        kv_copy(o).start()

    row_ids = lax.broadcasted_iota(jnp.int32, (rows, rows), 0)
    lane_ids = lax.broadcasted_iota(jnp.int32, (rows, rows), 1)

    def place_down(block):
        first = block[rows : rows + 1, :rows].astype(jnp.float32).astype(jnp.int32)
        second = block[rows + 1 : rows + 2, :rows].astype(jnp.float32).astype(jnp.int32)
        stretch = jnp.where(row_ids < half, first, second)
        return stretch * half + lax.rem(row_ids, half)

    own = kv_ref[...]
    first = own[rows : rows + 1, :rows].astype(jnp.float32).astype(jnp.int32)
    second = own[rows + 1 : rows + 2, :rows].astype(jnp.float32).astype(jnp.int32)
    place_across = jnp.where(lane_ids < half, first, second) * half + lax.rem(lane_ids, half)

    def gather_step(o):
        there = peer(o)
        mine, other = 2 * there + core, 2 * there + 1 - core

        def first_steps():
            if isinstance(o, int) and o == 0:
                kv_arrived(partner)
            else:
                kv_arrived(mine)
                kv_pass(o).start()
                kv_arrived(other)

        if isinstance(o, int):
            first_steps()
        else:
            kv_arrived(mine)
            kv_pass(o).start()
            kv_arrived(other)
        a, b = kv_all[mine], kv_all[other]
        k = jnp.concatenate([a[:rows, :head], b[:rows, :head]], axis=0)
        v = jnp.concatenate([a[:rows, head:], b[:rows, head:]], axis=0)
        visible = jnp.concatenate(
            [place_down(a) <= place_across, place_down(b) <= place_across], axis=0
        )
        visible = jnp.concatenate([visible] * group, axis=1)
        scores = dot(k, q_turned[...], ((1,), (0,))) * (scale * LOG2E)
        dprob = dot(v, g_turned[...], ((1,), (0,)))
        scores = jnp.where(visible, scores, hidden)
        block_top = jnp.max(scores, axis=0, keepdims=True)
        if isinstance(o, int) and o == 0:
            top = block_top
            e = jnp.exp2(scores - top)
            row_total[...] = jnp.sum(e, axis=0, keepdims=True)
            row_delta[...] = jnp.sum(e * dprob, axis=0, keepdims=True)
        else:
            old = row_top[...]
            top = jnp.maximum(old, block_top)
            fading = jnp.exp2(old - top)
            e = jnp.exp2(scores - top)
            row_total[...] = row_total[...] * fading + jnp.sum(e, axis=0, keepdims=True)
            row_delta[...] = row_delta[...] * fading + jnp.sum(e * dprob, axis=0, keepdims=True)
        row_top[...] = top
        tops[o] = top
        exps[o] = e
        dprobs[o] = dprob

    gather_step(0)
    if chips <= 4:
        for o in range(1, chips):
            gather_step(o)
    else:
        lax.fori_loop(1, chips, lambda o, c: (gather_step(o), c)[1], 0)

    inverse = 1.0 / row_total[...]
    delta = row_delta[...] * inverse
    last_top = row_top[...]
    dq_turned[...] = jnp.zeros_like(dq_turned)

    def pair_copy(o):
        return pltpu.make_async_remote_copy(
            src_ref=pair_send.at[o],
            dst_ref=pair_recv.at[o],
            send_sem=pair_send_sem.at[o],
            recv_sem=pair_recv_sem.at[o],
            device_id=(section, partner),
            device_id_type=MESH,
        )

    def sum_copy(o):
        return pltpu.make_async_remote_copy(
            src_ref=sum_send.at[o],
            dst_ref=sum_recv.at[chip],
            send_sem=sum_send_sem.at[o],
            recv_sem=sum_recv_sem.at[chip],
            device_id=(section, 2 * peer(o) + core),
            device_id_type=MESH,
        )

    def grad_step(o):
        there = peer(o)
        a, b = kv_all[2 * there + core], kv_all[2 * there + 1 - core]
        k = jnp.concatenate([a[:rows, :head], b[:rows, :head]], axis=0)
        fading = jnp.exp2(tops[o] - last_top) * inverse
        weights = exps[o] * fading
        probs = weights.astype(jnp.bfloat16)
        dscore = (weights * ((dprobs[o] - delta) * scale)).astype(jnp.bfloat16)
        dk = dot(dscore, q_rows[...], ((1,), (0,)))
        dv = dot(probs, g_rows[...], ((1,), (0,)))
        part = jnp.concatenate([dk, dv], axis=1)
        pair_send[o] = part[rows:].astype(jnp.bfloat16)
        pair_copy(o).start()
        own_part[o] = part[:rows]
        dq_turned[...] += dot(k, dscore, ((0,), (0,)))

    def sum_step(o):
        pair_copy(o).wait_recv()
        sum_send[o] = (own_part[o] + pair_recv[o].astype(jnp.float32)).astype(jnp.bfloat16)
        sum_copy(o).start()

    grad_step(chips - 1)
    if chips <= 4:
        for o in reversed(range(chips - 1)):
            grad_step(o)
            sum_step(o + 1)
    else:

        def both(i, c):
            o = chips - 2 - i
            grad_step(o)
            sum_step(o + 1)
            return c

        lax.fori_loop(0, chips - 1, both, 0)

    for h in range(group):
        at = slice(h * rows, (h + 1) * rows)
        message[:, h * head : (h + 1) * head] = dq_turned[:, at].T.astype(jnp.bfloat16)

    def relay(which, columns):
        return pltpu.make_async_remote_copy(
            src_ref=message.at[:, columns],
            dst_ref=out_ref.at[:, columns],
            send_sem=relay_send_sem.at[which],
            recv_sem=relay_recv_sem.at[which],
            device_id=(before, me),
            device_id_type=MESH,
        )

    width = group * head
    relay_q = relay(0, slice(0, width))
    relay_kv = relay(1, slice(width, width + 2 * head))
    relay_q.start()

    pair_copy(0).wait_recv()
    total = own_part[0] + pair_recv[0].astype(jnp.float32)

    def take(o, total):
        there = peer(o)
        pltpu.make_async_remote_copy(
            src_ref=sum_send.at[0],
            dst_ref=sum_recv.at[there],
            send_sem=sum_send_sem.at[0],
            recv_sem=sum_recv_sem.at[there],
            device_id=(section, partner),
            device_id_type=MESH,
        ).wait_recv()
        return total + sum_recv[there].astype(jnp.float32)

    if chips <= 4:
        for o in reversed(range(1, chips)):
            total = take(o, total)
    else:
        total = lax.fori_loop(1, chips, take, total)
    message[:, width:] = total.astype(jnp.bfloat16)
    relay_kv.start()

    kv_partner().wait_send()
    pair_copy(0).wait_send()

    def finish(o):
        kv_copy(o).wait_send()
        kv_pass(o).wait_send()
        pair_copy(o).wait_send()
        sum_copy(o).wait_send()

    if chips <= 4:
        for o in range(1, chips):
            finish(o)
    else:
        lax.fori_loop(1, chips, lambda o, c: (finish(o), c)[1], 0)
    relay_q.wait()
    relay_kv.wait()


def per_device(sections, n, queries, keys, values, out_grad, stretch_ids, stash_slot):
    slot = stash_slot[0]
    q = lax.dynamic_index_in_dim(queries[0], slot, 0, keepdims=False)
    k = lax.dynamic_index_in_dim(keys[0], slot, 0, keepdims=False)
    v = lax.dynamic_index_in_dim(values[0], slot, 0, keepdims=False)
    g = out_grad[0]
    rows, head = k.shape
    width = q.shape[1]
    group = width // head
    chips = n // 2
    marks = jnp.broadcast_to(stretch_ids.astype(jnp.bfloat16)[:, None], (2, 2 * head))
    kv = jnp.concatenate(
        [jnp.concatenate([k, v], axis=1), jnp.pad(marks, ((0, 14), (0, 0)))], axis=0
    )
    bf16, f32 = jnp.bfloat16, jnp.float32
    all_rows = group * rows
    block = (chips, rows, 2 * head)
    dma = pltpu.SemaphoreType.DMA
    out = pl.pallas_call(
        functools.partial(kernel, n, sections),
        out_shape=jax.ShapeDtypeStruct((rows, width + 2 * head), bf16),
        in_specs=[
            pl.BlockSpec(memory_space=pltpu.VMEM),
            pl.BlockSpec(memory_space=pl.ANY),
            pl.BlockSpec(memory_space=pl.ANY),
        ],
        out_specs=pl.BlockSpec(memory_space=pltpu.VMEM),
        scratch_shapes=[
            pltpu.VMEM((rows, width), bf16),
            pltpu.VMEM((rows, width), bf16),
            pltpu.VMEM((all_rows, head), bf16),
            pltpu.VMEM((all_rows, head), bf16),
            pltpu.VMEM((head, all_rows), bf16),
            pltpu.VMEM((head, all_rows), bf16),
            pltpu.VMEM((n,) + kv.shape, bf16),
            pltpu.VMEM((chips, 2 * rows, all_rows), f32),
            pltpu.VMEM((chips, 2 * rows, all_rows), f32),
            pltpu.VMEM((chips, 1, all_rows), f32),
            pltpu.VMEM((1, all_rows), f32),
            pltpu.VMEM((1, all_rows), f32),
            pltpu.VMEM((1, all_rows), f32),
            pltpu.VMEM((head, all_rows), f32),
            pltpu.VMEM(block, f32),
            pltpu.VMEM(block, bf16),
            pltpu.VMEM(block, bf16),
            pltpu.VMEM(block, bf16),
            pltpu.VMEM(block, bf16),
            pltpu.VMEM((rows, width + 2 * head), bf16),
            dma((2,)),
            dma((chips,)),
            dma((chips,)),
            dma((n,)),
            dma((chips,)),
            dma((chips,)),
            dma((chips,)),
            dma((chips,)),
            dma((2,)),
            dma((2,)),
        ],
        compiler_params=pltpu.CompilerParams(
            collective_id=0, has_side_effects=True, vmem_limit_bytes=60 * 1024 * 1024
        ),
    )(kv, q, g)
    return out[None]


def solution(mesh):
    in_specs = (
        P("section", None, "ctx", None),
        P("section", None, "ctx", None),
        P("section", None, "ctx", None),
        P("section", "ctx", None),
        P("ctx"),
        P("section"),
    )
    out_specs = P("section", "ctx", None)
    body = functools.partial(per_device, mesh.shape["section"], mesh.shape["ctx"])
    return jax.shard_map(
        body, mesh=mesh, in_specs=in_specs, out_specs=out_specs, check_vma=False
    )
```

```python
import functools
import math

import jax
import jax.numpy as jnp
from jax import lax
from jax.experimental import pallas as pl
from jax.experimental.pallas import tpu as pltpu
from jax.sharding import PartitionSpec as P

MESH = pl.DeviceIdType.MESH
LOG2E = 1.4426950408889634
hidden = -1e30


def dot(a, b, dims):
    return lax.dot_general(a, b, (dims, ((), ())), preferred_element_type=jnp.float32)


def paired_chip(chip, offset, chips):
    if chips & (chips - 1):
        return lax.rem(2 * chips + offset - chip, chips)
    result = chip
    bit = 1
    while bit < chips:
        result = result + ((offset // bit) % 2) * bit * (1 - 2 * ((chip // bit) % 2))
        bit *= 2
    return result


def over(count, body, backwards=False):
    if count <= 4:
        for step in reversed(range(count)) if backwards else range(count):
            body(step)
    else:
        lax.fori_loop(
            0, count, lambda i, c: (body(count - 1 - i if backwards else i), c)[1], 0
        )


def kernel(
    n,
    sections,
    slot_hbm,
    stretch_hbm,
    q_hbm,
    k_hbm,
    v_hbm,
    g_hbm,
    out_ref,
    slot_ref,
    stretch_ref,
    q_in,
    k_in,
    v_in,
    g_in,
    kv_ref,
    q_rows,
    g_rows,
    q_turned,
    g_turned,
    kv_all,
    exps,
    dprobs,
    tops,
    row_top,
    row_total,
    row_delta,
    dq_turned,
    own_part,
    pair_send,
    pair_recv,
    sum_send,
    sum_recv,
    message,
    load_sem,
    kv_send_sem,
    kv_pass_sem,
    kv_recv_sem,
    pair_send_sem,
    pair_recv_sem,
    sum_send_sem,
    sum_recv_sem,
    relay_send_sem,
    relay_recv_sem,
):
    chips = n // 2
    rows = kv_ref.shape[0] - 16
    head = kv_ref.shape[1] // 2
    group = g_hbm.shape[1] // head
    half = rows // 2
    scale = 1.0 / math.sqrt(head)
    me = lax.axis_index("ctx")
    section = lax.axis_index("section")
    core = lax.rem(me, 2)
    chip = me // 2
    partner = 2 * chip + 1 - core
    before = lax.rem(section + sections - 1, sections)
    after = lax.rem(section + 1, sections)

    def peer(offset):
        return paired_chip(chip, offset, chips)

    load_k = pltpu.make_async_copy(k_hbm, k_in, load_sem.at[0])
    load_v = pltpu.make_async_copy(v_hbm, v_in, load_sem.at[1])
    load_q = pltpu.make_async_copy(q_hbm, q_in, load_sem.at[2])
    load_g = pltpu.make_async_copy(g_hbm, g_in, load_sem.at[3])
    load_slot = pltpu.make_async_copy(slot_hbm, slot_ref, load_sem.at[4])
    load_stretch = pltpu.make_async_copy(stretch_hbm, stretch_ref, load_sem.at[5])
    load_slot.start()
    load_stretch.start()
    load_k.start()
    load_v.start()
    load_q.start()
    load_g.start()

    barrier = pltpu.get_barrier_semaphore()
    pl.semaphore_signal(barrier, inc=1, device_id=(section, partner), device_id_type=MESH)
    for o in range(1, chips):
        pl.semaphore_signal(
            barrier, inc=1, device_id=(section, 2 * peer(o) + core), device_id_type=MESH
        )
    pl.semaphore_signal(barrier, inc=1, device_id=(before, me), device_id_type=MESH)
    pl.semaphore_signal(barrier, inc=1, device_id=(after, me), device_id_type=MESH)

    load_slot.wait()
    load_stretch.wait()
    slot = slot_ref[0]
    load_k.wait()
    load_v.wait()
    kv_ref[:rows, :head] = k_in[slot]
    kv_ref[:rows, head:] = v_in[slot]
    mark_ids = lax.broadcasted_iota(jnp.int32, (16, 2 * head), 0)
    marks = jnp.where(mark_ids == 0, stretch_ref[0], stretch_ref[1])
    kv_ref[rows:, :] = marks.astype(jnp.float32).astype(jnp.bfloat16)

    pl.semaphore_wait(barrier, chips + 2)

    def kv_copy(o):
        return pltpu.make_async_remote_copy(
            src_ref=kv_ref,
            dst_ref=kv_all.at[me],
            send_sem=kv_send_sem.at[o],
            recv_sem=kv_recv_sem.at[me],
            device_id=(section, 2 * peer(o) + core),
            device_id_type=MESH,
        )

    def kv_partner():
        return pltpu.make_async_remote_copy(
            src_ref=kv_ref,
            dst_ref=kv_all.at[me],
            send_sem=kv_send_sem.at[0],
            recv_sem=kv_recv_sem.at[me],
            device_id=(section, partner),
            device_id_type=MESH,
        )

    def kv_pass(o):
        origin = 2 * peer(o) + core
        return pltpu.make_async_remote_copy(
            src_ref=kv_all.at[origin],
            dst_ref=kv_all.at[origin],
            send_sem=kv_pass_sem.at[o],
            recv_sem=kv_recv_sem.at[origin],
            device_id=(section, partner),
            device_id_type=MESH,
        )

    def kv_arrived(origin):
        pltpu.make_async_remote_copy(
            src_ref=kv_ref,
            dst_ref=kv_all.at[origin],
            send_sem=kv_send_sem.at[0],
            recv_sem=kv_recv_sem.at[origin],
            device_id=(section, partner),
            device_id_type=MESH,
        ).wait_recv()

    kv_partner().start()
    for o in range(1, chips):
        kv_copy(o).start()

    load_q.wait()
    load_g.wait()
    q_own = q_in[slot]
    for h in range(group):
        at = slice(h * rows, (h + 1) * rows)
        col = slice(h * head, (h + 1) * head)
        q_rows[at, :] = q_own[:, col]
        g_rows[at, :] = g_in[:, col]
        q_turned[:, at] = q_own[:, col].T
        g_turned[:, at] = g_in[:, col].T
    kv_all[me] = kv_ref[...]

    row_ids = lax.broadcasted_iota(jnp.int32, (rows, rows), 0)
    lane_ids = lax.broadcasted_iota(jnp.int32, (rows, rows), 1)

    def place_down(block):
        first = block[rows : rows + 1, :rows].astype(jnp.float32).astype(jnp.int32)
        second = block[rows + 1 : rows + 2, :rows].astype(jnp.float32).astype(jnp.int32)
        stretch = jnp.where(row_ids < half, first, second)
        return stretch * half + lax.rem(row_ids, half)

    own = kv_ref[...]
    first = own[rows : rows + 1, :rows].astype(jnp.float32).astype(jnp.int32)
    second = own[rows + 1 : rows + 2, :rows].astype(jnp.float32).astype(jnp.int32)
    place_across = jnp.where(lane_ids < half, first, second) * half + lax.rem(lane_ids, half)

    def gather_step(o):
        there = peer(o)
        mine, other = 2 * there + core, 2 * there + 1 - core

        def first_steps():
            if isinstance(o, int) and o == 0:
                kv_arrived(partner)
            else:
                kv_arrived(mine)
                kv_pass(o).start()
                kv_arrived(other)

        if isinstance(o, int):
            first_steps()
        else:
            kv_arrived(mine)
            kv_pass(o).start()
            kv_arrived(other)
        a, b = kv_all[mine], kv_all[other]
        k = jnp.concatenate([a[:rows, :head], b[:rows, :head]], axis=0)
        v = jnp.concatenate([a[:rows, head:], b[:rows, head:]], axis=0)
        visible = jnp.concatenate(
            [place_down(a) <= place_across, place_down(b) <= place_across], axis=0
        )
        visible = jnp.concatenate([visible] * group, axis=1)
        scores = dot(k, q_turned[...], ((1,), (0,))) * (scale * LOG2E)
        dprob = dot(v, g_turned[...], ((1,), (0,)))
        scores = jnp.where(visible, scores, hidden)
        block_top = jnp.max(scores, axis=0, keepdims=True)
        if isinstance(o, int) and o == 0:
            top = block_top
            e = jnp.exp2(scores - top)
            row_total[...] = jnp.sum(e, axis=0, keepdims=True)
            row_delta[...] = jnp.sum(e * dprob, axis=0, keepdims=True)
        else:
            old = row_top[...]
            top = jnp.maximum(old, block_top)
            fading = jnp.exp2(old - top)
            e = jnp.exp2(scores - top)
            row_total[...] = row_total[...] * fading + jnp.sum(e, axis=0, keepdims=True)
            row_delta[...] = row_delta[...] * fading + jnp.sum(e * dprob, axis=0, keepdims=True)
        row_top[...] = top
        tops[o] = top
        exps[o] = e
        dprobs[o] = dprob

    gather_step(0)
    if chips <= 4:
        for o in range(1, chips):
            gather_step(o)
    else:
        lax.fori_loop(1, chips, lambda o, c: (gather_step(o), c)[1], 0)

    inverse = 1.0 / row_total[...]
    delta = row_delta[...] * inverse
    last_top = row_top[...]
    dq_turned[...] = jnp.zeros_like(dq_turned)

    def pair_copy(o):
        return pltpu.make_async_remote_copy(
            src_ref=pair_send.at[o],
            dst_ref=pair_recv.at[o],
            send_sem=pair_send_sem.at[o],
            recv_sem=pair_recv_sem.at[o],
            device_id=(section, partner),
            device_id_type=MESH,
        )

    def sum_copy(o):
        return pltpu.make_async_remote_copy(
            src_ref=sum_send.at[o],
            dst_ref=sum_recv.at[chip],
            send_sem=sum_send_sem.at[o],
            recv_sem=sum_recv_sem.at[chip],
            device_id=(section, 2 * peer(o) + core),
            device_id_type=MESH,
        )

    def grad_step(o):
        there = peer(o)
        a, b = kv_all[2 * there + core], kv_all[2 * there + 1 - core]
        k = jnp.concatenate([a[:rows, :head], b[:rows, :head]], axis=0)
        fading = jnp.exp2(tops[o] - last_top) * inverse
        weights = exps[o] * fading
        probs = weights.astype(jnp.bfloat16)
        dscore = (weights * ((dprobs[o] - delta) * scale)).astype(jnp.bfloat16)
        dk = dot(dscore, q_rows[...], ((1,), (0,)))
        dv = dot(probs, g_rows[...], ((1,), (0,)))
        part = jnp.concatenate([dk, dv], axis=1)
        pair_send[o] = part[rows:].astype(jnp.bfloat16)
        pair_copy(o).start()
        own_part[o] = part[:rows]
        dq_turned[...] += dot(k, dscore, ((0,), (0,)))

    def sum_step(o):
        pair_copy(o).wait_recv()
        sum_send[o] = (own_part[o] + pair_recv[o].astype(jnp.float32)).astype(jnp.bfloat16)
        sum_copy(o).start()

    grad_step(chips - 1)
    if chips <= 4:
        for o in reversed(range(chips - 1)):
            grad_step(o)
            sum_step(o + 1)
    else:

        def both(i, c):
            o = chips - 2 - i
            grad_step(o)
            sum_step(o + 1)
            return c

        lax.fori_loop(0, chips - 1, both, 0)

    for h in range(group):
        at = slice(h * rows, (h + 1) * rows)
        message[:, h * head : (h + 1) * head] = dq_turned[:, at].T.astype(jnp.bfloat16)

    def relay(which, columns):
        return pltpu.make_async_remote_copy(
            src_ref=message.at[:, columns],
            dst_ref=out_ref.at[:, columns],
            send_sem=relay_send_sem.at[which],
            recv_sem=relay_recv_sem.at[which],
            device_id=(before, me),
            device_id_type=MESH,
        )

    width = group * head
    relay_q = relay(0, slice(0, width))
    relay_kv = relay(1, slice(width, width + 2 * head))
    relay_q.start()

    pair_copy(0).wait_recv()
    total = own_part[0] + pair_recv[0].astype(jnp.float32)

    def take(o, total):
        there = peer(o)
        pltpu.make_async_remote_copy(
            src_ref=sum_send.at[0],
            dst_ref=sum_recv.at[there],
            send_sem=sum_send_sem.at[0],
            recv_sem=sum_recv_sem.at[there],
            device_id=(section, partner),
            device_id_type=MESH,
        ).wait_recv()
        return total + sum_recv[there].astype(jnp.float32)

    if chips <= 4:
        for o in reversed(range(1, chips)):
            total = take(o, total)
    else:
        total = lax.fori_loop(1, chips, take, total)
    message[:, width:] = total.astype(jnp.bfloat16)
    relay_kv.start()

    kv_partner().wait_send()
    pair_copy(0).wait_send()

    def finish(o):
        kv_copy(o).wait_send()
        kv_pass(o).wait_send()
        pair_copy(o).wait_send()
        sum_copy(o).wait_send()

    if chips <= 4:
        for o in range(1, chips):
            finish(o)
    else:
        lax.fori_loop(1, chips, lambda o, c: (finish(o), c)[1], 0)
    relay_q.wait()
    relay_kv.wait()


def per_device(sections, n, queries, keys, values, out_grad, stretch_ids, stash_slot):
    slots, rows, head = keys.shape[1:]
    width = queries.shape[3]
    group = width // head
    chips = n // 2
    bf16, f32 = jnp.bfloat16, jnp.float32
    all_rows = group * rows
    block = (chips, rows, 2 * head)
    dma = pltpu.SemaphoreType.DMA
    out = pl.pallas_call(
        functools.partial(kernel, n, sections),
        out_shape=jax.ShapeDtypeStruct((rows, width + 2 * head), bf16),
        in_specs=[
            pl.BlockSpec(memory_space=pltpu.HBM),
            pl.BlockSpec(memory_space=pltpu.HBM),
            pl.BlockSpec(memory_space=pltpu.HBM),
            pl.BlockSpec(memory_space=pltpu.HBM),
            pl.BlockSpec(memory_space=pltpu.HBM),
            pl.BlockSpec(memory_space=pltpu.HBM),
        ],
        out_specs=pl.BlockSpec(memory_space=pl.ANY),
        scratch_shapes=[
            pltpu.SMEM((1,), jnp.int32),
            pltpu.SMEM((2,), jnp.int32),
            pltpu.VMEM((slots, rows, width), bf16),
            pltpu.VMEM((slots, rows, head), bf16),
            pltpu.VMEM((slots, rows, head), bf16),
            pltpu.VMEM((rows, width), bf16),
            pltpu.VMEM((rows + 16, 2 * head), bf16),
            pltpu.VMEM((all_rows, head), bf16),
            pltpu.VMEM((all_rows, head), bf16),
            pltpu.VMEM((head, all_rows), bf16),
            pltpu.VMEM((head, all_rows), bf16),
            pltpu.VMEM((n, rows + 16, 2 * head), bf16),
            pltpu.VMEM((chips, 2 * rows, all_rows), f32),
            pltpu.VMEM((chips, 2 * rows, all_rows), f32),
            pltpu.VMEM((chips, 1, all_rows), f32),
            pltpu.VMEM((1, all_rows), f32),
            pltpu.VMEM((1, all_rows), f32),
            pltpu.VMEM((1, all_rows), f32),
            pltpu.VMEM((head, all_rows), f32),
            pltpu.VMEM(block, f32),
            pltpu.VMEM(block, bf16),
            pltpu.VMEM(block, bf16),
            pltpu.VMEM(block, bf16),
            pltpu.VMEM(block, bf16),
            pltpu.VMEM((rows, width + 2 * head), bf16),
            dma((6,)),
            dma((chips,)),
            dma((chips,)),
            dma((n,)),
            dma((chips,)),
            dma((chips,)),
            dma((chips,)),
            dma((chips,)),
            dma((2,)),
            dma((2,)),
        ],
        compiler_params=pltpu.CompilerParams(
            collective_id=0, has_side_effects=True, vmem_limit_bytes=67043328
        ),
    )(stash_slot, stretch_ids, queries[0], keys[0], values[0], out_grad[0])
    return out[None]


def solution(mesh):
    in_specs = (
        P("section", None, "ctx", None),
        P("section", None, "ctx", None),
        P("section", None, "ctx", None),
        P("section", "ctx", None),
        P("ctx"),
        P("section"),
    )
    out_specs = P("section", "ctx", None)
    body = functools.partial(per_device, mesh.shape["section"], mesh.shape["ctx"])
    return jax.shard_map(
        body, mesh=mesh, in_specs=in_specs, out_specs=out_specs, check_vma=False
    )
```

```python
import functools
import math

import jax
import jax.numpy as jnp
from jax import lax
from jax.experimental import pallas as pl
from jax.experimental.pallas import tpu as pltpu
from jax.sharding import PartitionSpec as P

MESH = pl.DeviceIdType.MESH
LOG2E = 1.4426950408889634
hidden = -1e30


def dot(a, b, dims):
    return lax.dot_general(a, b, (dims, ((), ())), preferred_element_type=jnp.float32)


def paired_chip(chip, offset, chips):
    if chips & (chips - 1):
        return lax.rem(2 * chips + offset - chip, chips)
    result = chip
    bit = 1
    while bit < chips:
        result = result + ((offset // bit) % 2) * bit * (1 - 2 * ((chip // bit) % 2))
        bit *= 2
    return result


def over(count, body, backwards=False):
    if count <= 4:
        for step in reversed(range(count)) if backwards else range(count):
            body(step)
    else:
        lax.fori_loop(
            0, count, lambda i, c: (body(count - 1 - i if backwards else i), c)[1], 0
        )


def kernel(
    n,
    sections,
    slot_hbm,
    stretch_hbm,
    q_hbm,
    k_hbm,
    v_hbm,
    g_hbm,
    out_ref,
    slot_ref,
    stretch_ref,
    q_in,
    k_in,
    v_in,
    g_in,
    kv_ref,
    q_rows,
    g_rows,
    q_turned,
    g_turned,
    kv_all,
    exps,
    dprobs,
    tops,
    row_top,
    row_total,
    row_delta,
    dq_turned,
    own_part,
    pair_send,
    pair_recv,
    sum_send,
    sum_recv,
    far_recv,
    message,
    near_sum,
    relayed,
    out_kv,
    load_sem,
    kv_send_sem,
    kv_pass_sem,
    kv_recv_sem,
    pair_send_sem,
    pair_recv_sem,
    sum_send_sem,
    sum_recv_sem,
    far_recv_sem,
    relay_send_sem,
    relay_recv_sem,
):
    chips = n // 2
    rows = kv_ref.shape[0] - 16
    head = kv_ref.shape[1] // 2
    group = g_hbm.shape[1] // head
    half = rows // 2
    scale = 1.0 / math.sqrt(head)
    me = lax.axis_index("ctx")
    section = lax.axis_index("section")
    core = lax.rem(me, 2)
    chip = me // 2
    partner = 2 * chip + 1 - core
    before = lax.rem(section + sections - 1, sections)
    after = lax.rem(section + 1, sections)

    def peer(offset):
        return paired_chip(chip, offset, chips)

    far = tuple(range(max(chips - 2, 1), chips))

    load_k = pltpu.make_async_copy(k_hbm, k_in, load_sem.at[0])
    load_v = pltpu.make_async_copy(v_hbm, v_in, load_sem.at[1])
    load_q = pltpu.make_async_copy(q_hbm, q_in, load_sem.at[2])
    load_g = pltpu.make_async_copy(g_hbm, g_in, load_sem.at[3])
    load_slot = pltpu.make_async_copy(slot_hbm, slot_ref, load_sem.at[4])
    load_stretch = pltpu.make_async_copy(stretch_hbm, stretch_ref, load_sem.at[5])
    load_slot.start()
    load_stretch.start()
    load_k.start()
    load_v.start()
    load_q.start()
    load_g.start()

    barrier = pltpu.get_barrier_semaphore()
    pl.semaphore_signal(barrier, inc=1, device_id=(section, partner), device_id_type=MESH)
    for o in range(1, chips):
        pl.semaphore_signal(
            barrier, inc=1, device_id=(section, 2 * peer(o) + core), device_id_type=MESH
        )
    pl.semaphore_signal(barrier, inc=1, device_id=(after, me), device_id_type=MESH)
    for o in far:
        pl.semaphore_signal(
            barrier, inc=1, device_id=(after, 2 * peer(o) + core), device_id_type=MESH
        )

    load_slot.wait()
    load_stretch.wait()
    slot = slot_ref[0]
    load_k.wait()
    load_v.wait()
    kv_ref[:rows, :head] = k_in[slot]
    kv_ref[:rows, head:] = v_in[slot]
    mark_ids = lax.broadcasted_iota(jnp.int32, (16, 2 * head), 0)
    marks = jnp.where(mark_ids == 0, stretch_ref[0], stretch_ref[1])
    kv_ref[rows:, :] = marks.astype(jnp.float32).astype(jnp.bfloat16)

    pl.semaphore_wait(barrier, chips + 1 + len(far))

    def kv_copy(o):
        return pltpu.make_async_remote_copy(
            src_ref=kv_ref,
            dst_ref=kv_all.at[me],
            send_sem=kv_send_sem.at[o],
            recv_sem=kv_recv_sem.at[me],
            device_id=(section, 2 * peer(o) + core),
            device_id_type=MESH,
        )

    def kv_partner():
        return pltpu.make_async_remote_copy(
            src_ref=kv_ref,
            dst_ref=kv_all.at[me],
            send_sem=kv_send_sem.at[0],
            recv_sem=kv_recv_sem.at[me],
            device_id=(section, partner),
            device_id_type=MESH,
        )

    def kv_pass(o):
        origin = 2 * peer(o) + core
        return pltpu.make_async_remote_copy(
            src_ref=kv_all.at[origin],
            dst_ref=kv_all.at[origin],
            send_sem=kv_pass_sem.at[o],
            recv_sem=kv_recv_sem.at[origin],
            device_id=(section, partner),
            device_id_type=MESH,
        )

    def kv_arrived(origin):
        pltpu.make_async_remote_copy(
            src_ref=kv_ref,
            dst_ref=kv_all.at[origin],
            send_sem=kv_send_sem.at[0],
            recv_sem=kv_recv_sem.at[origin],
            device_id=(section, partner),
            device_id_type=MESH,
        ).wait_recv()

    kv_partner().start()
    for o in range(1, chips):
        kv_copy(o).start()

    load_q.wait()
    load_g.wait()
    q_own = q_in[slot]
    for h in range(group):
        at = slice(h * rows, (h + 1) * rows)
        col = slice(h * head, (h + 1) * head)
        q_rows[at, :] = q_own[:, col]
        g_rows[at, :] = g_in[:, col]
        q_turned[:, at] = q_own[:, col].T
        g_turned[:, at] = g_in[:, col].T
    kv_all[me] = kv_ref[...]

    row_ids = lax.broadcasted_iota(jnp.int32, (rows, rows), 0)
    lane_ids = lax.broadcasted_iota(jnp.int32, (rows, rows), 1)

    def place_down(block):
        first = block[rows : rows + 1, :rows].astype(jnp.float32).astype(jnp.int32)
        second = block[rows + 1 : rows + 2, :rows].astype(jnp.float32).astype(jnp.int32)
        stretch = jnp.where(row_ids < half, first, second)
        return stretch * half + lax.rem(row_ids, half)

    own = kv_ref[...]
    first = own[rows : rows + 1, :rows].astype(jnp.float32).astype(jnp.int32)
    second = own[rows + 1 : rows + 2, :rows].astype(jnp.float32).astype(jnp.int32)
    place_across = jnp.where(lane_ids < half, first, second) * half + lax.rem(lane_ids, half)

    def gather_step(o):
        there = peer(o)
        mine, other = 2 * there + core, 2 * there + 1 - core

        def first_steps():
            if isinstance(o, int) and o == 0:
                kv_arrived(partner)
            else:
                kv_arrived(mine)
                kv_pass(o).start()
                kv_arrived(other)

        if isinstance(o, int):
            first_steps()
        else:
            kv_arrived(mine)
            kv_pass(o).start()
            kv_arrived(other)
        a, b = kv_all[mine], kv_all[other]
        k = jnp.concatenate([a[:rows, :head], b[:rows, :head]], axis=0)
        v = jnp.concatenate([a[:rows, head:], b[:rows, head:]], axis=0)
        visible = jnp.concatenate(
            [place_down(a) <= place_across, place_down(b) <= place_across], axis=0
        )
        visible = jnp.concatenate([visible] * group, axis=1)
        scores = dot(k, q_turned[...], ((1,), (0,))) * (scale * LOG2E)
        dprob = dot(v, g_turned[...], ((1,), (0,)))
        scores = jnp.where(visible, scores, hidden)
        block_top = jnp.max(scores, axis=0, keepdims=True)
        if isinstance(o, int) and o == 0:
            top = block_top
            e = jnp.exp2(scores - top)
            row_total[...] = jnp.sum(e, axis=0, keepdims=True)
            row_delta[...] = jnp.sum(e * dprob, axis=0, keepdims=True)
        else:
            old = row_top[...]
            top = jnp.maximum(old, block_top)
            fading = jnp.exp2(old - top)
            e = jnp.exp2(scores - top)
            row_total[...] = row_total[...] * fading + jnp.sum(e, axis=0, keepdims=True)
            row_delta[...] = row_delta[...] * fading + jnp.sum(e * dprob, axis=0, keepdims=True)
        row_top[...] = top
        tops[o] = top
        exps[o] = e
        dprobs[o] = dprob

    gather_step(0)
    if chips <= 4:
        for o in range(1, chips):
            gather_step(o)
    else:
        lax.fori_loop(1, chips, lambda o, c: (gather_step(o), c)[1], 0)

    inverse = 1.0 / row_total[...]
    delta = row_delta[...] * inverse
    last_top = row_top[...]
    dq_turned[...] = jnp.zeros_like(dq_turned)

    def pair_copy(o):
        return pltpu.make_async_remote_copy(
            src_ref=pair_send.at[o],
            dst_ref=pair_recv.at[o],
            send_sem=pair_send_sem.at[o],
            recv_sem=pair_recv_sem.at[o],
            device_id=(section, partner),
            device_id_type=MESH,
        )

    def sum_copy(o):
        if isinstance(o, int) and o in far:
            return pltpu.make_async_remote_copy(
                src_ref=sum_send.at[o],
                dst_ref=far_recv.at[o - far[0]],
                send_sem=sum_send_sem.at[o],
                recv_sem=far_recv_sem.at[o - far[0]],
                device_id=(before, 2 * peer(o) + core),
                device_id_type=MESH,
            )
        return pltpu.make_async_remote_copy(
            src_ref=sum_send.at[o],
            dst_ref=sum_recv.at[chip],
            send_sem=sum_send_sem.at[o],
            recv_sem=sum_recv_sem.at[chip],
            device_id=(section, 2 * peer(o) + core),
            device_id_type=MESH,
        )

    def grad_step(o):
        there = peer(o)
        a, b = kv_all[2 * there + core], kv_all[2 * there + 1 - core]
        k = jnp.concatenate([a[:rows, :head], b[:rows, :head]], axis=0)
        fading = jnp.exp2(tops[o] - last_top) * inverse
        weights = exps[o] * fading
        probs = weights.astype(jnp.bfloat16)
        dscore = (weights * ((dprobs[o] - delta) * scale)).astype(jnp.bfloat16)
        dk = dot(dscore, q_rows[...], ((1,), (0,)))
        dv = dot(probs, g_rows[...], ((1,), (0,)))
        part = jnp.concatenate([dk, dv], axis=1)
        pair_send[o] = part[rows:].astype(jnp.bfloat16)
        pair_copy(o).start()
        own_part[o] = part[:rows]
        dq_turned[...] += dot(k, dscore, ((0,), (0,)))

    def sum_step(o):
        pair_copy(o).wait_recv()
        sum_send[o] = (own_part[o] + pair_recv[o].astype(jnp.float32)).astype(jnp.bfloat16)
        sum_copy(o).start()

    if chips <= 4:
        order = (3, 2, 1, 0) if chips == 4 else tuple(reversed(range(chips)))
        for place, o in enumerate(order):
            grad_step(o)
            if place:
                sum_step(order[place - 1])
    else:
        grad_step(chips - 1)
        for o in reversed(far):
            grad_step(o - 1)
            sum_step(o)

        def both(i, c):
            o = far[0] - 2 - i
            grad_step(o)
            sum_step(o + 1)
            return c

        lax.fori_loop(0, far[0] - 1, both, 0)

    for h in range(group):
        at = slice(h * rows, (h + 1) * rows)
        message[:, h * head : (h + 1) * head] = dq_turned[:, at].T.astype(jnp.bfloat16)

    width = group * head
    relay_q = pltpu.make_async_remote_copy(
        src_ref=message,
        dst_ref=out_ref.at[:, :width],
        send_sem=relay_send_sem.at[0],
        recv_sem=relay_recv_sem.at[0],
        device_id=(before, me),
        device_id_type=MESH,
    )
    relay_kv = pltpu.make_async_remote_copy(
        src_ref=near_sum,
        dst_ref=relayed,
        send_sem=relay_send_sem.at[1],
        recv_sem=relay_recv_sem.at[1],
        device_id=(before, me),
        device_id_type=MESH,
    )
    relay_q.start()

    pair_copy(0).wait_recv()
    total = own_part[0] + pair_recv[0].astype(jnp.float32)

    def take(o, total):
        there = peer(o)
        pltpu.make_async_remote_copy(
            src_ref=sum_send.at[0],
            dst_ref=sum_recv.at[there],
            send_sem=sum_send_sem.at[0],
            recv_sem=sum_recv_sem.at[there],
            device_id=(section, partner),
            device_id_type=MESH,
        ).wait_recv()
        return total + sum_recv[there].astype(jnp.float32)

    if chips <= 4:
        for o in range(1, far[0]):
            total = take(o, total)
    else:
        total = lax.fori_loop(1, far[0], take, total)
    near_sum[...] = total.astype(jnp.bfloat16)
    relay_kv.start()

    kv_partner().wait_send()
    pair_copy(0).wait_send()

    def finish(o):
        kv_copy(o).wait_send()
        kv_pass(o).wait_send()
        pair_copy(o).wait_send()
        sum_copy(o).wait_send()

    if chips > 4:
        lax.fori_loop(1, far[0], lambda o, c: (finish(o), c)[1], 0)
    for o in far if chips > 4 else range(1, chips):
        finish(o)

    relay_kv.wait()
    total = relayed[...].astype(jnp.float32)
    for o in far:
        sum_copy(o).wait_recv()
        total = total + far_recv[o - far[0]].astype(jnp.float32)
    out_kv[...] = total.astype(jnp.bfloat16)
    store = pltpu.make_async_copy(out_kv, out_ref.at[:, width:], load_sem.at[0])
    store.start()
    relay_q.wait()
    store.wait()


def per_device(sections, n, queries, keys, values, out_grad, stretch_ids, stash_slot):
    slots, rows, head = keys.shape[1:]
    width = queries.shape[3]
    group = width // head
    chips = n // 2
    bf16, f32 = jnp.bfloat16, jnp.float32
    all_rows = group * rows
    block = (chips, rows, 2 * head)
    dma = pltpu.SemaphoreType.DMA
    out = pl.pallas_call(
        functools.partial(kernel, n, sections),
        out_shape=jax.ShapeDtypeStruct((rows, width + 2 * head), bf16),
        in_specs=[
            pl.BlockSpec(memory_space=pltpu.HBM),
            pl.BlockSpec(memory_space=pltpu.HBM),
            pl.BlockSpec(memory_space=pltpu.HBM),
            pl.BlockSpec(memory_space=pltpu.HBM),
            pl.BlockSpec(memory_space=pltpu.HBM),
            pl.BlockSpec(memory_space=pltpu.HBM),
        ],
        out_specs=pl.BlockSpec(memory_space=pl.ANY),
        scratch_shapes=[
            pltpu.SMEM((1,), jnp.int32),
            pltpu.SMEM((2,), jnp.int32),
            pltpu.VMEM((slots, rows, width), bf16),
            pltpu.VMEM((slots, rows, head), bf16),
            pltpu.VMEM((slots, rows, head), bf16),
            pltpu.VMEM((rows, width), bf16),
            pltpu.VMEM((rows + 16, 2 * head), bf16),
            pltpu.VMEM((all_rows, head), bf16),
            pltpu.VMEM((all_rows, head), bf16),
            pltpu.VMEM((head, all_rows), bf16),
            pltpu.VMEM((head, all_rows), bf16),
            pltpu.VMEM((n, rows + 16, 2 * head), bf16),
            pltpu.VMEM((chips, 2 * rows, all_rows), f32),
            pltpu.VMEM((chips, 2 * rows, all_rows), f32),
            pltpu.VMEM((chips, 1, all_rows), f32),
            pltpu.VMEM((1, all_rows), f32),
            pltpu.VMEM((1, all_rows), f32),
            pltpu.VMEM((1, all_rows), f32),
            pltpu.VMEM((head, all_rows), f32),
            pltpu.VMEM(block, f32),
            pltpu.VMEM(block, bf16),
            pltpu.VMEM(block, bf16),
            pltpu.VMEM(block, bf16),
            pltpu.VMEM(block, bf16),
            pltpu.VMEM((2, rows, 2 * head), bf16),
            pltpu.VMEM((rows, width), bf16),
            pltpu.VMEM((rows, 2 * head), bf16),
            pltpu.VMEM((rows, 2 * head), bf16),
            pltpu.VMEM((rows, 2 * head), bf16),
            dma((6,)),
            dma((chips,)),
            dma((chips,)),
            dma((n,)),
            dma((chips,)),
            dma((chips,)),
            dma((chips,)),
            dma((chips,)),
            dma((2,)),
            dma((2,)),
            dma((2,)),
        ],
        compiler_params=pltpu.CompilerParams(
            collective_id=0, has_side_effects=True, vmem_limit_bytes=67043328
        ),
    )(stash_slot, stretch_ids, queries[0], keys[0], values[0], out_grad[0])
    return out[None]


def solution(mesh):
    in_specs = (
        P("section", None, "ctx", None),
        P("section", None, "ctx", None),
        P("section", None, "ctx", None),
        P("section", "ctx", None),
        P("ctx"),
        P("section"),
    )
    out_specs = P("section", "ctx", None)
    body = functools.partial(per_device, mesh.shape["section"], mesh.shape["ctx"])
    return jax.shard_map(
        body, mesh=mesh, in_specs=in_specs, out_specs=out_specs, check_vma=False
    )
```

```python
import functools
import math

import jax
import jax.numpy as jnp
from jax import lax
from jax.experimental import pallas as pl
from jax.experimental.pallas import tpu as pltpu
from jax.sharding import PartitionSpec as P

MESH = pl.DeviceIdType.MESH
LOG2E = 1.4426950408889634
hidden = -1e30


def dot(a, b, dims):
    return lax.dot_general(a, b, (dims, ((), ())), preferred_element_type=jnp.float32)


def paired_chip(chip, offset, chips):
    if chips & (chips - 1):
        return lax.rem(2 * chips + offset - chip, chips)
    result = chip
    bit = 1
    while bit < chips:
        result = result + ((offset // bit) % 2) * bit * (1 - 2 * ((chip // bit) % 2))
        bit *= 2
    return result


def over(count, body, backwards=False):
    if count <= 4:
        for step in reversed(range(count)) if backwards else range(count):
            body(step)
    else:
        lax.fori_loop(
            0, count, lambda i, c: (body(count - 1 - i if backwards else i), c)[1], 0
        )


def kernel(
    n,
    sections,
    slot_hbm,
    stretch_hbm,
    q_hbm,
    k_hbm,
    v_hbm,
    g_hbm,
    out_ref,
    slot_ref,
    stretch_ref,
    q_in,
    k_in,
    v_in,
    g_in,
    kv_ref,
    q_rows,
    g_rows,
    q_turned,
    g_turned,
    kv_all,
    exps,
    dprobs,
    tops,
    row_top,
    row_total,
    row_delta,
    dq_turned,
    own_part,
    pair_send,
    pair_recv,
    sum_send,
    sum_recv,
    far_recv,
    message,
    near_sum,
    relayed,
    out_kv,
    load_sem,
    kv_send_sem,
    kv_pass_sem,
    kv_recv_sem,
    pair_send_sem,
    pair_recv_sem,
    sum_send_sem,
    sum_recv_sem,
    far_recv_sem,
    relay_send_sem,
    relay_recv_sem,
):
    chips = n // 2
    rows = kv_ref.shape[0] - 16
    head = kv_ref.shape[1] // 2
    group = g_hbm.shape[1] // head
    half = rows // 2
    scale = 1.0 / math.sqrt(head)
    me = lax.axis_index("ctx")
    section = lax.axis_index("section")
    core = lax.rem(me, 2)
    chip = me // 2
    partner = 2 * chip + 1 - core
    before = lax.rem(section + sections - 1, sections)
    after = lax.rem(section + 1, sections)

    def peer(offset):
        return paired_chip(chip, offset, chips)

    far = tuple(range(max(chips - 2, 1), chips))

    load_k = pltpu.make_async_copy(k_hbm, k_in, load_sem.at[0])
    load_v = pltpu.make_async_copy(v_hbm, v_in, load_sem.at[1])
    load_q = pltpu.make_async_copy(q_hbm, q_in, load_sem.at[2])
    load_g = pltpu.make_async_copy(g_hbm, g_in, load_sem.at[3])
    load_slot = pltpu.make_async_copy(slot_hbm, slot_ref, load_sem.at[4])
    load_stretch = pltpu.make_async_copy(stretch_hbm, stretch_ref, load_sem.at[5])
    load_slot.start()
    load_stretch.start()
    load_k.start()
    load_v.start()
    load_q.start()
    load_g.start()

    barrier = pltpu.get_barrier_semaphore()
    pl.semaphore_signal(barrier, inc=1, device_id=(section, partner), device_id_type=MESH)
    for o in range(1, chips):
        pl.semaphore_signal(
            barrier, inc=1, device_id=(section, 2 * peer(o) + core), device_id_type=MESH
        )
    pl.semaphore_signal(barrier, inc=1, device_id=(after, me), device_id_type=MESH)
    for o in far:
        pl.semaphore_signal(
            barrier, inc=1, device_id=(after, 2 * peer(o) + core), device_id_type=MESH
        )

    load_slot.wait()
    load_stretch.wait()
    slot = slot_ref[0]
    load_k.wait()
    load_v.wait()
    kv_ref[:rows, :head] = k_in[slot]
    kv_ref[:rows, head:] = v_in[slot]
    mark_ids = lax.broadcasted_iota(jnp.int32, (16, 2 * head), 0)
    marks = jnp.where(mark_ids == 0, stretch_ref[0], stretch_ref[1])
    kv_ref[rows:, :] = marks.astype(jnp.float32).astype(jnp.bfloat16)

    pl.semaphore_wait(barrier, chips + 1 + len(far))

    def kv_copy(o):
        return pltpu.make_async_remote_copy(
            src_ref=kv_ref,
            dst_ref=kv_all.at[me],
            send_sem=kv_send_sem.at[o],
            recv_sem=kv_recv_sem.at[me],
            device_id=(section, 2 * peer(o) + core),
            device_id_type=MESH,
        )

    def kv_partner():
        return pltpu.make_async_remote_copy(
            src_ref=kv_ref,
            dst_ref=kv_all.at[me],
            send_sem=kv_send_sem.at[0],
            recv_sem=kv_recv_sem.at[me],
            device_id=(section, partner),
            device_id_type=MESH,
        )

    def kv_pass(o):
        origin = 2 * peer(o) + core
        return pltpu.make_async_remote_copy(
            src_ref=kv_all.at[origin],
            dst_ref=kv_all.at[origin],
            send_sem=kv_pass_sem.at[o],
            recv_sem=kv_recv_sem.at[origin],
            device_id=(section, partner),
            device_id_type=MESH,
        )

    def kv_arrived(origin):
        pltpu.make_async_remote_copy(
            src_ref=kv_ref,
            dst_ref=kv_all.at[origin],
            send_sem=kv_send_sem.at[0],
            recv_sem=kv_recv_sem.at[origin],
            device_id=(section, partner),
            device_id_type=MESH,
        ).wait_recv()

    kv_partner().start()
    for o in range(1, chips):
        kv_copy(o).start()

    load_q.wait()
    load_g.wait()
    q_own = q_in[slot]
    for h in range(group):
        at = slice(h * rows, (h + 1) * rows)
        col = slice(h * head, (h + 1) * head)
        q_rows[at, :] = q_own[:, col]
        g_rows[at, :] = g_in[:, col]
        q_turned[:, at] = q_own[:, col].T
        g_turned[:, at] = g_in[:, col].T
    kv_all[me] = kv_ref[...]

    row_ids = lax.broadcasted_iota(jnp.int32, (rows, rows), 0)
    lane_ids = lax.broadcasted_iota(jnp.int32, (rows, rows), 1)

    def place_down(block):
        first = block[rows : rows + 1, :rows].astype(jnp.float32).astype(jnp.int32)
        second = block[rows + 1 : rows + 2, :rows].astype(jnp.float32).astype(jnp.int32)
        stretch = jnp.where(row_ids < half, first, second)
        return stretch * half + lax.rem(row_ids, half)

    own = kv_ref[...]
    first = own[rows : rows + 1, :rows].astype(jnp.float32).astype(jnp.int32)
    second = own[rows + 1 : rows + 2, :rows].astype(jnp.float32).astype(jnp.int32)
    place_across = jnp.where(lane_ids < half, first, second) * half + lax.rem(lane_ids, half)

    def gather_step(o):
        there = peer(o)
        mine, other = 2 * there + core, 2 * there + 1 - core

        def first_steps():
            if isinstance(o, int) and o == 0:
                kv_arrived(partner)
            else:
                kv_arrived(mine)
                kv_pass(o).start()
                kv_arrived(other)

        if isinstance(o, int):
            first_steps()
        else:
            kv_arrived(mine)
            kv_pass(o).start()
            kv_arrived(other)
        a, b = kv_all[mine], kv_all[other]
        k = jnp.concatenate([a[:rows, :head], b[:rows, :head]], axis=0)
        v = jnp.concatenate([a[:rows, head:], b[:rows, head:]], axis=0)
        visible = jnp.concatenate(
            [place_down(a) <= place_across, place_down(b) <= place_across], axis=0
        )
        visible = jnp.concatenate([visible] * group, axis=1)
        scores = dot(k, q_turned[...], ((1,), (0,))) * (scale * LOG2E)
        dprob = dot(v, g_turned[...], ((1,), (0,)))
        scores = jnp.where(visible, scores, hidden)
        block_top = jnp.max(scores, axis=0, keepdims=True)
        if isinstance(o, int) and o == 0:
            top = block_top
            e = jnp.exp2(scores - top)
            row_total[...] = jnp.sum(e, axis=0, keepdims=True)
            row_delta[...] = jnp.sum(e * dprob, axis=0, keepdims=True)
        else:
            old = row_top[...]
            top = jnp.maximum(old, block_top)
            fading = jnp.exp2(old - top)
            e = jnp.exp2(scores - top)
            row_total[...] = row_total[...] * fading + jnp.sum(e, axis=0, keepdims=True)
            row_delta[...] = row_delta[...] * fading + jnp.sum(e * dprob, axis=0, keepdims=True)
        row_top[...] = top
        tops[o] = top
        exps[o] = e
        dprobs[o] = dprob

    gather_step(0)
    if chips <= 4:
        for o in range(1, chips):
            gather_step(o)
    else:
        lax.fori_loop(1, chips, lambda o, c: (gather_step(o), c)[1], 0)

    inverse = 1.0 / row_total[...]
    delta = row_delta[...] * inverse
    last_top = row_top[...]
    dq_turned[...] = jnp.zeros_like(dq_turned)

    def pair_copy(o):
        return pltpu.make_async_remote_copy(
            src_ref=pair_send.at[o],
            dst_ref=pair_recv.at[o],
            send_sem=pair_send_sem.at[o],
            recv_sem=pair_recv_sem.at[o],
            device_id=(section, partner),
            device_id_type=MESH,
        )

    def sum_copy(o):
        if isinstance(o, int) and o in far:
            return pltpu.make_async_remote_copy(
                src_ref=sum_send.at[o],
                dst_ref=far_recv.at[o - far[0]],
                send_sem=sum_send_sem.at[o],
                recv_sem=far_recv_sem.at[o - far[0]],
                device_id=(before, 2 * peer(o) + core),
                device_id_type=MESH,
            )
        return pltpu.make_async_remote_copy(
            src_ref=sum_send.at[o],
            dst_ref=sum_recv.at[chip],
            send_sem=sum_send_sem.at[o],
            recv_sem=sum_recv_sem.at[chip],
            device_id=(section, 2 * peer(o) + core),
            device_id_type=MESH,
        )

    def grad_step(o):
        there = peer(o)
        a, b = kv_all[2 * there + core], kv_all[2 * there + 1 - core]
        k = jnp.concatenate([a[:rows, :head], b[:rows, :head]], axis=0)
        fading = jnp.exp2(tops[o] - last_top) * inverse
        weights = exps[o] * fading
        probs = weights.astype(jnp.bfloat16)
        dscore = (weights * ((dprobs[o] - delta) * scale)).astype(jnp.bfloat16)
        dk = dot(dscore, q_rows[...], ((1,), (0,)))
        dv = dot(probs, g_rows[...], ((1,), (0,)))
        part = jnp.concatenate([dk, dv], axis=1)
        pair_send[o] = part[rows:].astype(jnp.bfloat16)
        pair_copy(o).start()
        own_part[o] = part[:rows]
        dq_turned[...] += dot(k, dscore, ((0,), (0,)))

    def sum_step(o):
        pair_copy(o).wait_recv()
        sum_send[o] = (own_part[o] + pair_recv[o].astype(jnp.float32)).astype(jnp.bfloat16)
        sum_copy(o).start()

    if chips <= 4:
        order = (3, 2, 1, 0) if chips == 4 else tuple(reversed(range(chips)))
        for place, o in enumerate(order):
            grad_step(o)
            if place:
                sum_step(order[place - 1])
    else:
        grad_step(chips - 1)
        for o in reversed(far):
            grad_step(o - 1)
            sum_step(o)

        def both(i, c):
            o = far[0] - 2 - i
            grad_step(o)
            sum_step(o + 1)
            return c

        lax.fori_loop(0, far[0] - 1, both, 0)

    for h in range(group):
        at = slice(h * rows, (h + 1) * rows)
        message[:, h * head : (h + 1) * head] = dq_turned[:, at].T.astype(jnp.bfloat16)

    width = group * head
    relay_q = pltpu.make_async_remote_copy(
        src_ref=message,
        dst_ref=out_ref.at[:, :width],
        send_sem=relay_send_sem.at[0],
        recv_sem=relay_recv_sem.at[0],
        device_id=(before, me),
        device_id_type=MESH,
    )
    relay_kv = pltpu.make_async_remote_copy(
        src_ref=near_sum,
        dst_ref=relayed,
        send_sem=relay_send_sem.at[1],
        recv_sem=relay_recv_sem.at[1],
        device_id=(before, me),
        device_id_type=MESH,
    )
    relay_q.start()

    pair_copy(0).wait_recv()
    total = own_part[0] + pair_recv[0].astype(jnp.float32)

    def take(o, total):
        there = peer(o)
        pltpu.make_async_remote_copy(
            src_ref=sum_send.at[0],
            dst_ref=sum_recv.at[there],
            send_sem=sum_send_sem.at[0],
            recv_sem=sum_recv_sem.at[there],
            device_id=(section, partner),
            device_id_type=MESH,
        ).wait_recv()
        return total + sum_recv[there].astype(jnp.float32)

    if chips <= 4:
        for o in range(1, far[0]):
            total = take(o, total)
    else:
        total = lax.fori_loop(1, far[0], take, total)
    near_sum[...] = total.astype(jnp.bfloat16)
    relay_kv.start()

    kv_partner().wait_send()
    pair_copy(0).wait_send()

    def finish(o):
        kv_copy(o).wait_send()
        kv_pass(o).wait_send()
        pair_copy(o).wait_send()
        sum_copy(o).wait_send()

    if chips > 4:
        lax.fori_loop(1, far[0], lambda o, c: (finish(o), c)[1], 0)
    for o in far if chips > 4 else range(1, chips):
        finish(o)

    relay_kv.wait()
    total = relayed[...].astype(jnp.float32)
    for o in far:
        sum_copy(o).wait_recv()
        total = total + far_recv[o - far[0]].astype(jnp.float32)
    out_kv[...] = total.astype(jnp.bfloat16)
    store = pltpu.make_async_copy(out_kv, out_ref.at[:, width:], load_sem.at[0])
    store.start()
    relay_q.wait()
    store.wait()


def per_device(sections, n, queries, keys, values, out_grad, stretch_ids, stash_slot):
    slots, rows, head = keys.shape[1:]
    width = queries.shape[3]
    group = width // head
    chips = n // 2
    bf16, f32 = jnp.bfloat16, jnp.float32
    all_rows = group * rows
    block = (chips, rows, 2 * head)
    dma = pltpu.SemaphoreType.DMA
    out = pl.pallas_call(
        functools.partial(kernel, n, sections),
        out_shape=pltpu.VMEM((rows, width + 2 * head), bf16),
        in_specs=[
            pl.BlockSpec(memory_space=pltpu.HBM),
            pl.BlockSpec(memory_space=pltpu.HBM),
            pl.BlockSpec(memory_space=pltpu.HBM),
            pl.BlockSpec(memory_space=pltpu.HBM),
            pl.BlockSpec(memory_space=pltpu.HBM),
            pl.BlockSpec(memory_space=pltpu.HBM),
        ],
        out_specs=pl.BlockSpec(memory_space=pl.ANY),
        scratch_shapes=[
            pltpu.SMEM((1,), jnp.int32),
            pltpu.SMEM((2,), jnp.int32),
            pltpu.VMEM((slots, rows, width), bf16),
            pltpu.VMEM((slots, rows, head), bf16),
            pltpu.VMEM((slots, rows, head), bf16),
            pltpu.VMEM((rows, width), bf16),
            pltpu.VMEM((rows + 16, 2 * head), bf16),
            pltpu.VMEM((all_rows, head), bf16),
            pltpu.VMEM((all_rows, head), bf16),
            pltpu.VMEM((head, all_rows), bf16),
            pltpu.VMEM((head, all_rows), bf16),
            pltpu.VMEM((n, rows + 16, 2 * head), bf16),
            pltpu.VMEM((chips, 2 * rows, all_rows), f32),
            pltpu.VMEM((chips, 2 * rows, all_rows), f32),
            pltpu.VMEM((chips, 1, all_rows), f32),
            pltpu.VMEM((1, all_rows), f32),
            pltpu.VMEM((1, all_rows), f32),
            pltpu.VMEM((1, all_rows), f32),
            pltpu.VMEM((head, all_rows), f32),
            pltpu.VMEM(block, f32),
            pltpu.VMEM(block, bf16),
            pltpu.VMEM(block, bf16),
            pltpu.VMEM(block, bf16),
            pltpu.VMEM(block, bf16),
            pltpu.VMEM((2, rows, 2 * head), bf16),
            pltpu.VMEM((rows, width), bf16),
            pltpu.VMEM((rows, 2 * head), bf16),
            pltpu.VMEM((rows, 2 * head), bf16),
            pltpu.VMEM((rows, 2 * head), bf16),
            dma((6,)),
            dma((chips,)),
            dma((chips,)),
            dma((n,)),
            dma((chips,)),
            dma((chips,)),
            dma((chips,)),
            dma((chips,)),
            dma((2,)),
            dma((2,)),
            dma((2,)),
        ],
        compiler_params=pltpu.CompilerParams(
            collective_id=0, has_side_effects=True, vmem_limit_bytes=67043328 - (3 << 20)
        ),
    )(stash_slot, stretch_ids, queries[0], keys[0], values[0], out_grad[0])
    return out[None]


def solution(mesh):
    in_specs = (
        P("section", None, "ctx", None),
        P("section", None, "ctx", None),
        P("section", None, "ctx", None),
        P("section", "ctx", None),
        P("ctx"),
        P("section"),
    )
    out_specs = P("section", "ctx", None)
    body = functools.partial(per_device, mesh.shape["section"], mesh.shape["ctx"])
    return jax.shard_map(
        body, mesh=mesh, in_specs=in_specs, out_specs=out_specs, check_vma=False
    )
```
